8 devices in a mesh: dp: 1 (over z), tp: 2 (over y), cp: 4 (over x, core).
Axes of the slice: x: 2, y: 2, z: 1, core: 2. Of those that a mesh axis runs over, the one named last changes fastest.
Arguments:
- hidden: bfloat16 [2, 3072, 5376], P('dp', 'cp')
- cotangent: bfloat16 [2, 3072, 5376], P('dp', 'cp')
- positions: int32 [3072], P(('dp', 'cp'))
- w_q: bfloat16 [5376, 4096], P(None, 'tp')
- w_k: bfloat16 [5376, 2048], P(None, 'tp')
- w_v: bfloat16 [5376, 2048], P(None, 'tp')
- w_o: bfloat16 [4096, 5376], P('tp')
- w_pre: float32 [5376], replicated
- w_post: float32 [5376], replicated
- q_norm: float32 [128], replicated
- k_norm: float32 [128], replicated
Outputs:
- output 1: bfloat16 [2, 3072, 5376], P('dp', 'cp')
- output 2: bfloat16 [2, 3072, 5376], P('dp', 'cp')
- output 3: float32 [5376, 4096], P('dp', 'tp')
- output 4: float32 [5376, 2048], P('dp', 'tp')
- output 5: float32 [5376, 2048], P('dp', 'tp')
- output 6: float32 [4096, 5376], P(('dp', 'tp'))
- output 7: float32 [5376], P('dp')
- output 8: float32 [5376], P('dp')
- output 9: float32 [128], P('dp')
- output 10: float32 [128], P('dp')
All inputs are finite; a program needn't handle non-finite values.
Results may differ from the reference program's by a relative error of at most 0.02.
Values are sent between devices in bfloat16 or wider.
A program may use at most 1 GiB of HBM per device.

```python
import jax
import jax.numpy as jnp
from jax import lax

BATCH = 2
SEQ_LEN = 3072
MODEL_DIM = 5376
NUM_HEADS = 32
KV_HEADS = 16
HEAD_DIM = 128
CP_SIZE = 4
QUERY_BLOCK = 64
POS_RANGE = 131072

EPS = 1e-6
ROPE_BASE = 1000000.0
ROPE_SCALE = 8.0
NEG_BIG = -1e30


def draw_positions(key):
    gap_max = POS_RANGE // SEQ_LEN
    pos_gaps = jax.random.randint(key, (SEQ_LEN,), 1, gap_max + 1, dtype=jnp.int32)
    logical = jnp.cumsum(pos_gaps) - pos_gaps[0]
    piece_len = SEQ_LEN // (2 * CP_SIZE)
    pieces = logical.reshape(2 * CP_SIZE, piece_len)
    layout = jnp.stack([pieces[:CP_SIZE], pieces[CP_SIZE:][::-1]], axis=1)
    return layout.reshape(SEQ_LEN).astype(jnp.int32)


def setup_inputs(seed: int = 0, part: int = 0) -> dict:
    part_keys = jax.random.split(jax.random.fold_in(jax.random.key(seed), part), 3)
    weight_keys = jax.random.split(jax.random.key(seed + 1), 8)
    act_shape = (BATCH, SEQ_LEN, MODEL_DIM)
    q_cols = NUM_HEADS * HEAD_DIM
    kv_cols = KV_HEADS * HEAD_DIM
    hidden = jax.random.normal(part_keys[0], act_shape, jnp.float32).astype(jnp.bfloat16)
    cotangent = jax.random.normal(part_keys[1], act_shape, jnp.float32).astype(jnp.bfloat16)
    w_q = (jax.random.normal(weight_keys[0], (MODEL_DIM, q_cols), jnp.float32) * MODEL_DIM ** -0.5).astype(jnp.bfloat16)
    w_k = (jax.random.normal(weight_keys[1], (MODEL_DIM, kv_cols), jnp.float32) * MODEL_DIM ** -0.5).astype(jnp.bfloat16)
    w_v = (jax.random.normal(weight_keys[2], (MODEL_DIM, kv_cols), jnp.float32) * MODEL_DIM ** -0.5).astype(jnp.bfloat16)
    w_o = (jax.random.normal(weight_keys[3], (q_cols, MODEL_DIM), jnp.float32) * q_cols ** -0.5).astype(jnp.bfloat16)
    w_pre = 0.3 * jax.random.normal(weight_keys[4], (MODEL_DIM,), jnp.float32)
    w_post = 0.3 * jax.random.normal(weight_keys[5], (MODEL_DIM,), jnp.float32)
    q_norm = 0.3 * jax.random.normal(weight_keys[6], (HEAD_DIM,), jnp.float32)
    k_norm = 0.3 * jax.random.normal(weight_keys[7], (HEAD_DIM,), jnp.float32)
    return {'hidden': hidden, 'cotangent': cotangent, 'positions': draw_positions(part_keys[2]), 'w_q': w_q, 'w_k': w_k, 'w_v': w_v, 'w_o': w_o, 'w_pre': w_pre, 'w_post': w_post, 'q_norm': q_norm, 'k_norm': k_norm}


def rms_unit(values):
    return values * lax.rsqrt(jnp.mean(values * values, axis=-1, keepdims=True) + EPS)


def to_bf16(values):
    return values.astype(jnp.bfloat16).astype(jnp.float32)


def rope_apply(values, cos_t, sin_t):
    half_dim = values.shape[-1] // 2
    lower_half = values[..., :half_dim]
    upper_half = values[..., half_dim:]
    return jnp.concatenate([lower_half * cos_t - upper_half * sin_t, upper_half * cos_t + lower_half * sin_t], axis=-1)


def block_forward(x_f32, w_q, w_k, w_v, w_o, w_pre, w_post, q_norm, k_norm, positions):
    groups = NUM_HEADS // KV_HEADS
    normed = to_bf16(rms_unit(x_f32) * (1.0 + w_pre))
    q_raw = to_bf16(jnp.einsum('bsd,dh->bsh', normed, w_q)).reshape(BATCH, SEQ_LEN, NUM_HEADS, HEAD_DIM)
    k_raw = to_bf16(jnp.einsum('bsd,dh->bsh', normed, w_k)).reshape(BATCH, SEQ_LEN, KV_HEADS, HEAD_DIM)
    v_heads = to_bf16(jnp.einsum('bsd,dh->bsh', normed, w_v)).reshape(BATCH, SEQ_LEN, KV_HEADS, HEAD_DIM)
    half_dim = HEAD_DIM // 2
    inv_freq = 1.0 / (ROPE_SCALE * ROPE_BASE ** (jnp.arange(half_dim, dtype=jnp.float32) * (2.0 / HEAD_DIM)))
    angles = positions.astype(jnp.float32)[:, None] * inv_freq[None, :]
    cos_t = jnp.cos(angles)[None, :, None, :]
    sin_t = jnp.sin(angles)[None, :, None, :]
    q_fin = to_bf16(rope_apply(rms_unit(q_raw) * (1.0 + q_norm), cos_t, sin_t))
    k_fin = to_bf16(rope_apply(rms_unit(k_raw) * (1.0 + k_norm), cos_t, sin_t))
    score_scale = HEAD_DIM ** -0.5
    n_blocks = SEQ_LEN // QUERY_BLOCK
    q_blocks = jnp.moveaxis(q_fin.reshape(BATCH, n_blocks, QUERY_BLOCK, KV_HEADS, groups, HEAD_DIM), 1, 0)
    pos_blocks = positions.reshape(n_blocks, QUERY_BLOCK)

    def one_block(block_in):
        q_blk, q_pos = block_in
        scores = jnp.einsum('bqkgd,bskd->bkgqs', q_blk, k_fin) * score_scale
        allowed = positions[None, :] <= q_pos[:, None]
        attn_prob = jax.nn.softmax(jnp.where(allowed, scores, NEG_BIG), axis=-1)
        return jnp.einsum('bkgqs,bskd->bqkgd', attn_prob, v_heads)

    block_outs = lax.map(jax.checkpoint(one_block), (q_blocks, pos_blocks))
    attn_in = to_bf16(jnp.moveaxis(block_outs, 0, 1).reshape(BATCH, SEQ_LEN, NUM_HEADS * HEAD_DIM))
    attn = jnp.einsum('bsh,hd->bsd', attn_in, w_o)
    return x_f32 + rms_unit(attn) * (1.0 + w_post)


def reference(hidden, cotangent, positions, w_q, w_k, w_v, w_o, w_pre, w_post, q_norm, k_norm):
    def forward(x_f32, wq_f32, wk_f32, wv_f32, wo_f32, pre_gain, post_gain, q_gain, k_gain):
        return block_forward(x_f32, wq_f32, wk_f32, wv_f32, wo_f32, pre_gain, post_gain, q_gain, k_gain, positions)

    out_f32, pullback = jax.vjp(forward, hidden.astype(jnp.float32), w_q.astype(jnp.float32), w_k.astype(jnp.float32), w_v.astype(jnp.float32), w_o.astype(jnp.float32), w_pre, w_post, q_norm, k_norm)
    grad_list = pullback(cotangent.astype(jnp.float32))
    return (out_f32.astype(jnp.bfloat16), grad_list[0].astype(jnp.bfloat16), grad_list[1], grad_list[2], grad_list[3], grad_list[4], grad_list[5], grad_list[6], grad_list[7], grad_list[8])
```

```python
import functools

import jax
import jax.numpy as jnp
from jax import lax
from jax.experimental import pallas as pl
from jax.experimental.pallas import tpu as pltpu
from jax.sharding import PartitionSpec as P

EPS = 1e-6
ROPE_BASE = 1000000.0
ROPE_SCALE = 8.0
NEG_BIG = -1e30
LOG2E = 1.4426950408889634
VMEM_CAP = 60 * 1024 * 1024
F32 = jnp.float32
BF16 = jnp.bfloat16

S_DEV, S_TP, S_CORE, S_X, S_PEER, S_BLOCK = 0, 1, 2, 3, 4, 8

NN = (((1,), (0,)), ((), ()))
NT = (((1,), (1,)), ((), ()))
TN = (((0,), (0,)), ((), ()))


def mm(lhs, rhs, dims=NN):
    return lax.dot_general(lhs, rhs, dims, preferred_element_type=F32)


def params(n_grid, vmem=VMEM_CAP):
    sem = ("arbitrary",) * n_grid if n_grid else None
    return pltpu.CompilerParams(dimension_semantics=sem, vmem_limit_bytes=vmem)


def cost(flops, nbytes, trans=0):
    return pl.CostEstimate(flops=int(flops), bytes_accessed=int(nbytes), transcendentals=int(trans))


def qkv_kernel(s_ref, x_ref, wpre_ref, wq_ref, wk_ref, wv_ref, normed_ref, *outs):
    peer = pl.program_id(1)
    rows = normed_ref.shape[0]
    qw, kw = wq_ref.shape[1], wk_ref.shape[1]

    @pl.when(peer == 0)
    def _():
        gain = 1.0 + wpre_ref[...]

        def chunk(step, carry):
            here = pl.ds(pl.multiple_of(step * 16, 16), 16)
            xf = x_ref[0, here, :].astype(F32)
            inv = lax.rsqrt(jnp.mean(xf * xf, axis=-1, keepdims=True) + EPS)
            normed_ref[here, :] = (xf * inv * gain).astype(BF16)
            return carry

        lax.fori_loop(0, rows // 16, chunk, 0)

    normed = normed_ref[...]
    for rel in range(4):
        @pl.when(peer == rel)
        def _(out=outs[rel]):
            out[:, :qw] = mm(normed, wq_ref[...]).astype(BF16)
            out[:, qw:qw + kw] = mm(normed, wk_ref[...]).astype(BF16)
            out[:, qw + kw:] = mm(normed, wv_ref[...]).astype(BF16)


def project(table, hidden, w_pre, w_q, w_k, w_v, batch, n_blocks):
    _, seq, width = hidden.shape
    qw, kw = w_q.shape[1] // n_blocks, w_k.shape[1] // n_blocks
    tile = 384
    row = lambda t, r, s: (t, 0)
    col = lambda t, r, s: (0, s[S_BLOCK + r])
    block = qw + 2 * kw
    return pl.pallas_call(
        qkv_kernel,
        grid_spec=pltpu.PrefetchScalarGridSpec(
            num_scalar_prefetch=1,
            grid=(seq // tile, n_blocks),
            in_specs=[
                pl.BlockSpec((1, tile, width), lambda t, r, s: (batch, t, 0)),
                pl.BlockSpec((1, width), lambda t, r, s: (0, 0)),
                pl.BlockSpec((width, qw), col),
                pl.BlockSpec((width, kw), col),
                pl.BlockSpec((width, kw), col),
            ],
            out_specs=[pl.BlockSpec((tile, width), row)] + [pl.BlockSpec((tile, block), row)] * n_blocks,
        ),
        out_shape=[jax.ShapeDtypeStruct((seq, width), BF16)] + [jax.ShapeDtypeStruct((seq, block), BF16)] * n_blocks,
        compiler_params=params(2),
        cost_estimate=cost(2 * seq * width * block * n_blocks, 4 * seq * width + 4 * width * block * n_blocks),
        name="qkv",
    )(table, hidden, w_pre, w_q, w_k, w_v)


def rope_fwd(vals, cos2, sin2):
    return vals * cos2 + pltpu.roll(vals, vals.shape[-1] // 2, 1) * sin2


def rope_bwd(grads, cos2, sin2):
    return grads * cos2 - pltpu.roll(grads, grads.shape[-1] // 2, 1) * sin2


def unit_of(raw):
    vals = raw.astype(F32)
    inv = lax.rsqrt(jnp.mean(vals * vals, axis=-1, keepdims=True) + EPS)
    return vals * inv, inv


def final_head(raw, gain, cos2, sin2):
    unit, _ = unit_of(raw)
    return rope_fwd(unit * gain, cos2, sin2).astype(BF16)


def gather_pieces(s_ref, srcs, dst, sems, piece, n_dev):
    copies = []
    for rel, src in enumerate(srcs):
        peer = s_ref[S_PEER + rel]
        for half in range(2):
            where = peer if half == 0 else 2 * n_dev - 1 - peer
            copies.append(pltpu.make_async_copy(
                src.at[pl.ds(half * piece, piece)],
                dst.at[pl.ds(pl.multiple_of(where * piece, piece), piece)],
                sems.at[2 * rel + half]))
    return copies


def slot_of(piece_idx, n_dev):
    return jnp.where(piece_idx < n_dev, 2 * piece_idx, 4 * n_dev - 1 - 2 * piece_idx)


def causal_t(piece, groups):
    keys = lax.broadcasted_iota(jnp.int32, (piece, piece), 0)
    queries = lax.broadcasted_iota(jnp.int32, (piece, piece), 1)
    return jnp.concatenate([keys <= queries] * groups, axis=1)


def attend_kernel(s_ref, a0, a1, a2, a3, cos_ref, sin_ref, qg_ref, kg_ref, out_ref, lse_ref,
                  raw, kf, vt, qf, m_ref, l_ref, acc, sems, *, dim, kv, groups, piece, n_dev):
    qw, kw = kv * groups * dim, kv * dim
    n_piece = 2 * n_dev
    scale = dim ** -0.5 * LOG2E
    copies = gather_pieces(s_ref, (a0, a1, a2, a3), raw, sems, piece, n_dev)
    for copy in copies:
        copy.start()
    for copy in copies:
        copy.wait()
    k_gain = 1.0 + kg_ref[...]
    q_gain = 1.0 + qg_ref[...]

    def rows_of(idx):
        return pl.ds(pl.multiple_of(idx * piece, piece), piece)

    def prepare(idx, carry):
        here = rows_of(idx)
        cos2, sin2 = cos_ref[here, :], sin_ref[here, :]
        for h in range(kv):
            kf[h, here, :] = final_head(raw[here, qw + h * dim:qw + (h + 1) * dim], k_gain, cos2, sin2)
            vals = raw[here, qw + kw + h * dim:qw + kw + (h + 1) * dim]
            vt[h, :, here] = vals.astype(F32).T.astype(BF16)
        return carry

    lax.fori_loop(0, n_piece, prepare, 0)

    def block(idx, h, first, mask):
        here = rows_of(idx)
        sc = mm(kf[h, here, :], qf[h], NT) * scale
        if mask is not None:
            sc = jnp.where(mask, sc, NEG_BIG)
        top = jnp.max(sc, axis=0, keepdims=True)
        if first:
            new = top
        else:
            old = m_ref[h]
            new = jnp.maximum(old, top)
        prob = jnp.exp2(sc - new)
        tot = jnp.sum(prob, axis=0, keepdims=True)
        part = mm(vt[h, :, here], prob.astype(BF16))
        m_ref[h] = new
        if first:
            l_ref[h] = tot
            acc[h] = part
        else:
            fac = jnp.exp2(old - new)
            l_ref[h] = l_ref[h] * fac + tot
            acc[h] = acc[h] * fac + part

    def query_piece(p, carry):
        here = rows_of(p)
        cos2, sin2 = cos_ref[here, :], sin_ref[here, :]
        for h in range(kv):
            for g in range(groups):
                head = h * groups + g
                qf[h, g * piece:(g + 1) * piece, :] = final_head(
                    raw[here, head * dim:(head + 1) * dim], q_gain, cos2, sin2)
        mask = causal_t(piece, groups)
        for h in range(kv):
            block(p, h, True, mask)

        def inner(j, c):
            for h in range(kv):
                block(j, h, False, None)
            return c

        lax.fori_loop(0, p, inner, 0)
        there = rows_of(slot_of(p, n_dev))
        for h in range(kv):
            total = l_ref[h]
            o_t = acc[h] / total
            lse = m_ref[h] + jnp.log2(total)
            for g in range(groups):
                head = h * groups + g
                cols = slice(g * piece, (g + 1) * piece)
                out_ref[there, head * dim:(head + 1) * dim] = o_t[:, cols].T.astype(BF16)
                lse_ref[head:head + 1, here] = lse[:, cols]
        return carry

    lax.fori_loop(0, n_piece, query_piece, 0)


def attend(table, blocks, cos2, sin2, q_norm, k_norm, dim, kv, groups):
    seq = blocks[0].shape[0]
    n_dev = len(blocks)
    width = blocks[0].shape[1]
    total, piece, heads = seq * n_dev, seq // 2, kv * groups
    vm = pl.BlockSpec(memory_space=pltpu.VMEM)
    hbm = pl.BlockSpec(memory_space=pl.ANY)
    flops = 4 * heads * dim * total * total * 9 / 16
    return pl.pallas_call(
        functools.partial(attend_kernel, dim=dim, kv=kv, groups=groups, piece=piece, n_dev=n_dev),
        grid_spec=pltpu.PrefetchScalarGridSpec(
            num_scalar_prefetch=1, grid=(),
            in_specs=[hbm] * 4 + [vm] * 4, out_specs=[vm, vm],
            scratch_shapes=[
                pltpu.VMEM((total, width), BF16),
                pltpu.VMEM((kv, total, dim), BF16),
                pltpu.VMEM((kv, dim, total), BF16),
                pltpu.VMEM((kv, groups * piece, dim), BF16),
                pltpu.VMEM((kv, 1, groups * piece), F32),
                pltpu.VMEM((kv, 1, groups * piece), F32),
                pltpu.VMEM((kv, dim, groups * piece), F32),
                pltpu.SemaphoreType.DMA((8,)),
            ]),
        out_shape=[jax.ShapeDtypeStruct((total, heads * dim), BF16), jax.ShapeDtypeStruct((heads, total), F32)],
        compiler_params=params(0),
        cost_estimate=cost(2 * flops, 4 * total * width, heads * total * total // 2),
        name="attend",
    )(table, *blocks, cos2, sin2, q_norm, k_norm)


def attend_back_kernel(s_ref, a0, a1, a2, a3, g0, g1, g2, g3, o_hbm, lse_ref, cos_ref, sin_ref, qg_ref, kg_ref,
                       out_ref, gain_ref, raw, dout, o_ref, kf, kt, qf, dof, dk, dv, dqt, sems, *,
                       dim, kv, groups, piece, n_dev):
    qw, kw = kv * groups * dim, kv * dim
    n_piece = 2 * n_dev
    scale = dim ** -0.5
    copies = gather_pieces(s_ref, (a0, a1, a2, a3), raw, sems, piece, n_dev)
    copies += gather_pieces(s_ref, (g0, g1, g2, g3), dout, sems.at[pl.ds(8, 8)], piece, n_dev)
    copies.append(pltpu.make_async_copy(o_hbm, o_ref, sems.at[16]))
    for copy in copies:
        copy.start()
    for copy in copies:
        copy.wait()
    k_gain = 1.0 + kg_ref[...]
    q_gain = 1.0 + qg_ref[...]

    def rows_of(idx):
        return pl.ds(pl.multiple_of(idx * piece, piece), piece)

    def prepare(idx, carry):
        here = rows_of(idx)
        cos2, sin2 = cos_ref[here, :], sin_ref[here, :]
        for h in range(kv):
            unit, _ = unit_of(raw[here, qw + h * dim:qw + (h + 1) * dim])
            final = rope_fwd(unit * k_gain, cos2, sin2).astype(BF16)
            kf[h, here, :] = final
            kt[h, :, here] = final.astype(F32).T.astype(BF16)
        return carry

    lax.fori_loop(0, n_piece, prepare, 0)
    gain_ref[...] = jnp.zeros_like(gain_ref)

    def norm_back(d_final, raw_vals, gain, cos2, sin2, slot):
        unit, inv = unit_of(raw_vals)
        d_scaled = rope_bwd(d_final, cos2, sin2)
        gain_ref[slot:slot + 1, :] += jnp.sum(d_scaled * unit, axis=0, keepdims=True)
        d_unit = d_scaled * gain
        return (inv * (d_unit - unit * jnp.mean(d_unit * unit, axis=-1, keepdims=True))).astype(BF16)

    def query_piece(p, carry):
        here = rows_of(p)
        there = rows_of(slot_of(p, n_dev))
        cos2, sin2 = cos_ref[here, :], sin_ref[here, :]
        lse_rows, delta_rows = [], []
        for h in range(kv):
            lses, deltas = [], []
            for g in range(groups):
                head = h * groups + g
                cols = slice(head * dim, (head + 1) * dim)
                rows = slice(g * piece, (g + 1) * piece)
                qf[h, rows, :] = final_head(raw[here, cols], q_gain, cos2, sin2)
                d_o = dout[here, cols]
                dof[h, rows, :] = d_o
                prod = d_o.astype(F32) * o_ref[there, cols].astype(F32)
                deltas.append(jnp.sum(prod.T, axis=0, keepdims=True))
                lses.append(lse_ref[head:head + 1, here])
            lse_rows.append(jnp.concatenate(lses, axis=1))
            delta_rows.append(jnp.concatenate(deltas, axis=1))

        def block(idx, h, first, mask):
            keys = rows_of(idx)
            k_blk = kf[h, keys, :]
            v_blk = raw[keys, qw + kw + h * dim:qw + kw + (h + 1) * dim]
            q_all, do_all = qf[h], dof[h]
            prob = jnp.exp2(mm(k_blk, q_all, NT) * (scale * LOG2E) - lse_rows[h])
            if mask is not None:
                prob = jnp.where(mask, prob, 0.0)
            d_sc = (prob * (mm(v_blk, do_all, NT) - delta_rows[h])).astype(BF16)
            dv_part = mm(prob.astype(BF16), do_all)
            dk_part = mm(d_sc, q_all)
            dq_part = mm(kt[h, :, keys], d_sc)
            if first:
                dv[h, keys, :] = dv_part
                dk[h, keys, :] = dk_part
                dqt[h] = dq_part
            else:
                dv[h, keys, :] += dv_part
                dk[h, keys, :] += dk_part
                dqt[h] += dq_part

        mask = causal_t(piece, groups)
        for h in range(kv):
            block(p, h, True, mask)

        def inner(j, c):
            for h in range(kv):
                block(j, h, False, None)
            return c

        lax.fori_loop(0, p, inner, 0)
        for h in range(kv):
            for g in range(groups):
                head = h * groups + g
                cols = slice(head * dim, (head + 1) * dim)
                d_q = dqt[h, :, g * piece:(g + 1) * piece].T * scale
                out_ref[there, cols] = norm_back(d_q, raw[here, cols], q_gain, cos2, sin2, 0)
        return carry

    lax.fori_loop(0, n_piece, query_piece, 0)

    def finish(idx, carry):
        here = rows_of(idx)
        there = rows_of(slot_of(idx, n_dev))
        cos2, sin2 = cos_ref[here, :], sin_ref[here, :]
        for h in range(kv):
            cols = slice(qw + h * dim, qw + (h + 1) * dim)
            out_ref[there, cols] = norm_back(dk[h, here, :] * scale, raw[here, cols], k_gain, cos2, sin2, 1)
            out_ref[there, qw + kw + h * dim:qw + kw + (h + 1) * dim] = dv[h, here, :].astype(BF16)
        return carry

    lax.fori_loop(0, n_piece, finish, 0)


def attend_back(table, blocks, d_blocks, out, lse, cos2, sin2, q_norm, k_norm, dim, kv, groups):
    seq = blocks[0].shape[0]
    n_dev = len(blocks)
    width = blocks[0].shape[1]
    total, piece, heads = seq * n_dev, seq // 2, kv * groups
    vm = pl.BlockSpec(memory_space=pltpu.VMEM)
    hbm = pl.BlockSpec(memory_space=pl.ANY)
    flops = 10 * heads * dim * total * total * 9 / 16
    return pl.pallas_call(
        functools.partial(attend_back_kernel, dim=dim, kv=kv, groups=groups, piece=piece, n_dev=n_dev),
        grid_spec=pltpu.PrefetchScalarGridSpec(
            num_scalar_prefetch=1, grid=(),
            in_specs=[hbm] * 9 + [vm] * 5, out_specs=[vm, vm],
            scratch_shapes=[
                pltpu.VMEM((total, width), BF16),
                pltpu.VMEM((total, heads * dim), BF16),
                pltpu.VMEM((total, heads * dim), BF16),
                pltpu.VMEM((kv, total, dim), BF16),
                pltpu.VMEM((kv, dim, total), BF16),
                pltpu.VMEM((kv, groups * piece, dim), BF16),
                pltpu.VMEM((kv, groups * piece, dim), BF16),
                pltpu.VMEM((kv, total, dim), F32),
                pltpu.VMEM((kv, total, dim), F32),
                pltpu.VMEM((kv, dim, groups * piece), F32),
                pltpu.SemaphoreType.DMA((17,)),
            ]),
        out_shape=[jax.ShapeDtypeStruct((total, width), BF16), jax.ShapeDtypeStruct((8, dim), F32)],
        compiler_params=params(0),
        cost_estimate=cost(2 * flops, 6 * total * width, heads * total * total // 2),
        name="attend_back",
    )(table, *blocks, *d_blocks, out, lse, cos2, sin2, q_norm, k_norm)


def out_kernel(s_ref, own_ref, far_ref, w_own_ref, w_far_ref, x_ref, dy_ref, wpost_ref, *rest):
    y_ref, datt_ref, dpost_ref, acc = rest[-4:]
    step = pl.program_id(1)
    rows = acc.shape[0]

    @pl.when(step == 0)
    def _():
        acc[...] = mm(own_ref[...], w_own_ref[...])

    @pl.when((step > 0) & (step < 4))
    def _():
        acc[...] += mm(own_ref[...], w_own_ref[...])

    @pl.when(step >= 4)
    def _():
        acc[...] += mm(far_ref[...], w_far_ref[...])

    @pl.when(step == 7)
    def _():
        gain = 1.0 + wpost_ref[...]

        @pl.when(pl.program_id(0) == 0)
        def _():
            dpost_ref[...] = jnp.zeros_like(dpost_ref)

        def chunk(k, carry):
            here = pl.ds(pl.multiple_of(k * 16, 16), 16)
            vals = acc[here, :]
            inv = lax.rsqrt(jnp.mean(vals * vals, axis=-1, keepdims=True) + EPS)
            unit = vals * inv
            y_ref[0, here, :] = (x_ref[0, here, :].astype(F32) + unit * gain).astype(BF16)
            grad = dy_ref[0, here, :].astype(F32)
            prod = grad * unit
            dpost_ref[...] += prod[:8] + prod[8:]
            d_unit = grad * gain
            datt_ref[here, :] = (inv * (d_unit - unit * jnp.mean(d_unit * unit, axis=-1, keepdims=True))).astype(BF16)
            return carry

        lax.fori_loop(0, rows // 16, chunk, 0)


def project_out(table, own, far, w_own, w_far, hidden, cotangent, w_post, batch, y_prev):
    n_batch, seq, width = hidden.shape
    depth = own.shape[1] // 4
    tile = 384
    near = lambda t, k, s: (t, jnp.minimum(k, 3))
    away = lambda t, k, s: (t, jnp.maximum(k - 4, 0))

    def w_away(t, k, s):
        rel = jnp.maximum(k - 4, 0)
        return (2 * (rel % 2) + (s[S_X] + rel // 2) % 2, 0)

    once = pl.Buffered(1)
    act = lambda t, k, s: (batch, t, 0)
    in_specs = [
        pl.BlockSpec((tile, depth), near),
        pl.BlockSpec((tile, depth), away),
        pl.BlockSpec((depth, width), lambda t, k, s: (s[S_BLOCK + jnp.minimum(k, 3)], 0)),
        pl.BlockSpec((depth, width), w_away),
        pl.BlockSpec((1, tile, width), act, pipeline_mode=once),
        pl.BlockSpec((1, tile, width), act, pipeline_mode=once),
        pl.BlockSpec((1, width), lambda t, k, s: (0, 0)),
    ]
    args = [table, own, far, w_own, w_far, hidden, cotangent, w_post]
    alias = {}
    if y_prev is not None:
        in_specs.append(pl.BlockSpec(memory_space=pl.ANY))
        args.append(y_prev)
        alias = {8: 0}
    return pl.pallas_call(
        out_kernel,
        grid_spec=pltpu.PrefetchScalarGridSpec(
            num_scalar_prefetch=1, grid=(seq // tile, 8),
            in_specs=in_specs,
            out_specs=[
                pl.BlockSpec((1, tile, width), act),
                pl.BlockSpec((tile, width), lambda t, k, s: (t, 0)),
                pl.BlockSpec((8, width), lambda t, k, s: (0, 0)),
            ],
            scratch_shapes=[pltpu.VMEM((tile, width), F32)],
        ),
        out_shape=[jax.ShapeDtypeStruct((n_batch, seq, width), BF16), jax.ShapeDtypeStruct((seq, width), BF16),
                   jax.ShapeDtypeStruct((8, width), F32)],
        input_output_aliases=alias,
        compiler_params=params(2),
        cost_estimate=cost(2 * seq * width * depth * 8, 8 * seq * width + 32 * depth * width),
        name="project_out",
    )(*args)


def dout_kernel(s_ref, d_ref, w_ref, *outs):
    peer = pl.program_id(0)
    for rel in range(4):
        @pl.when(peer == rel)
        def _(out=outs[rel]):
            out[...] = mm(d_ref[...], w_ref[...], NT).astype(BF16)


def heads_grad(table, d_attn, w_o, n_blocks):
    seq, width = d_attn.shape
    depth = w_o.shape[0] // n_blocks
    tile = 384
    return pl.pallas_call(
        dout_kernel,
        grid_spec=pltpu.PrefetchScalarGridSpec(
            num_scalar_prefetch=1, grid=(n_blocks, seq // tile),
            in_specs=[pl.BlockSpec((tile, width), lambda r, t, s: (t, 0)),
                      pl.BlockSpec((depth, width), lambda r, t, s: (s[S_BLOCK + r], 0))],
            out_specs=[pl.BlockSpec((tile, depth), functools.partial(
                lambda r, t, s, rel: (jnp.where(r < rel, 0, jnp.where(r == rel, t, seq // tile - 1)), 0), rel=rel))
                for rel in range(n_blocks)],
        ),
        out_shape=[jax.ShapeDtypeStruct((seq, depth), BF16)] * n_blocks,
        compiler_params=params(2),
        cost_estimate=cost(2 * seq * width * depth * n_blocks, 2 * (seq * width * 4 + depth * width * n_blocks)),
        name="heads_grad",
    )(table, d_attn, w_o)


def din_kernel(s_ref, d0, d1, d2, d3, wq_ref, wk_ref, wv_ref, keep_ref, send_ref, dq, dk, dv):
    qw, kw = dq.shape[1] // 4, dk.shape[1] // 4
    half = keep_ref.shape[0]

    @pl.when(pl.program_id(0) == 0)
    def _():
        for rel, src in enumerate((d0, d1, d2, d3)):
            blk = s_ref[S_BLOCK + rel]
            for part in range(2):
                start = ((s_ref[S_TP] + part) % 2) * half
                rows = pl.ds(pl.multiple_of(start, half), half)
                to = slice(part * half, (part + 1) * half)
                dq[to, pl.ds(pl.multiple_of(blk * qw, qw), qw)] = src[rows, :qw]
                dk[to, pl.ds(pl.multiple_of(blk * kw, kw), kw)] = src[rows, qw:qw + kw]
                dv[to, pl.ds(pl.multiple_of(blk * kw, kw), kw)] = src[rows, qw + kw:]

    out = mm(dq[...], wq_ref[...], NT) + mm(dk[...], wk_ref[...], NT) + mm(dv[...], wv_ref[...], NT)
    keep_ref[...] = out[:half]
    send_ref[...] = out[half:]


def input_grad(table, grads, w_q, w_k, w_v, seq):
    width = w_q.shape[0]
    block = grads[0].shape[1]
    tile = 896
    return pl.pallas_call(
        din_kernel,
        grid_spec=pltpu.PrefetchScalarGridSpec(
            num_scalar_prefetch=1, grid=(width // tile,),
            in_specs=[pl.BlockSpec((seq, block), lambda n, s: (s[S_DEV], 0))] * 4 + [
                pl.BlockSpec((tile, w.shape[1]), lambda n, s: (n, 0)) for w in (w_q, w_k, w_v)],
            out_specs=[pl.BlockSpec((seq // 2, tile), lambda n, s: (0, n))] * 2,
            scratch_shapes=[pltpu.VMEM((seq, w.shape[1]), BF16) for w in (w_q, w_k, w_v)],
        ),
        out_shape=[jax.ShapeDtypeStruct((seq // 2, width), F32)] * 2,
        compiler_params=params(1),
        cost_estimate=cost(2 * seq * width * block * 4, 2 * width * block * 4 + 4 * seq * width),
        name="input_grad",
    )(table, *grads, w_q, w_k, w_v)


def dx_kernel(s_ref, keep_ref, got_ref, x_ref, dy_ref, wpre_ref, dx_ref, dpre_ref):
    gain = 1.0 + wpre_ref[...]

    @pl.when(pl.program_id(0) == 0)
    def _():
        dpre_ref[...] = jnp.zeros_like(dpre_ref)

    def chunk(k, carry):
        here = pl.ds(pl.multiple_of(k * 16, 16), 16)
        xf = x_ref[0, here, :].astype(F32)
        inv = lax.rsqrt(jnp.mean(xf * xf, axis=-1, keepdims=True) + EPS)
        unit = xf * inv
        d_normed = keep_ref[here, :] + got_ref[here, :]
        prod = d_normed * unit
        dpre_ref[...] += prod[:8] + prod[8:]
        d_unit = d_normed * gain
        back = inv * (d_unit - unit * jnp.mean(d_unit * unit, axis=-1, keepdims=True))
        dx_ref[here, :] = (dy_ref[0, here, :].astype(F32) + back).astype(BF16)
        return carry

    lax.fori_loop(0, keep_ref.shape[0] // 16, chunk, 0)


def finish_dx(table, keep, got, hidden, cotangent, w_pre, batch):
    half, width = keep.shape
    tile = 96
    steps = half // tile
    row = lambda t, s: (t, 0)
    act = lambda t, s: (batch, s[S_TP] * steps + t, 0)
    return pl.pallas_call(
        dx_kernel,
        grid_spec=pltpu.PrefetchScalarGridSpec(
            num_scalar_prefetch=1, grid=(steps,),
            in_specs=[pl.BlockSpec((tile, width), row), pl.BlockSpec((tile, width), row),
                      pl.BlockSpec((1, tile, width), act), pl.BlockSpec((1, tile, width), act),
                      pl.BlockSpec((1, width), lambda t, s: (0, 0))],
            out_specs=[pl.BlockSpec((tile, width), row), pl.BlockSpec((8, width), lambda t, s: (0, 0))],
        ),
        out_shape=[jax.ShapeDtypeStruct((half, width), BF16), jax.ShapeDtypeStruct((8, width), F32)],
        compiler_params=params(1),
        cost_estimate=cost(20 * half * width, 14 * half * width),
        name="finish_dx",
    )(table, keep, got, hidden, cotangent, w_pre)


def stream(pieces, col, buf, sems, step, slot):
    for idx, src in enumerate(pieces):
        @pl.when(step == idx)
        def _(src=src):
            pltpu.make_async_copy(src.at[:, col], buf.at[slot], sems.at[slot]).start()


def dw_in_kernel(s_ref, *refs):
    n_piece = 8
    pieces, grads = refs[:n_piece], refs[n_piece:n_piece + 2]
    wq_ref, wk_ref, wv_ref, buf, sems = refs[-5:]
    m_idx, step = pl.program_id(0), pl.program_id(1)
    tile = buf.shape[2]
    slot = (m_idx * n_piece + step) % 2
    qw, kw = wq_ref.shape[1], wk_ref.shape[1]

    def columns(m):
        return pl.ds(pl.multiple_of((s_ref[S_CORE] * pl.num_programs(0) + m) * tile, tile), tile)

    @pl.when((m_idx == 0) & (step == 0))
    def _():
        stream(pieces, columns(0), buf, sems, step, slot)

    @pl.when(step < n_piece - 1)
    def _():
        stream(pieces, columns(m_idx), buf, sems, step + 1, 1 - slot)

    @pl.when((step == n_piece - 1) & (m_idx < pl.num_programs(0) - 1))
    def _():
        stream(pieces, columns(m_idx + 1), buf, sems, 0, 1 - slot)

    pltpu.make_async_copy(pieces[0].at[:, columns(0)], buf.at[slot], sems.at[slot]).wait()
    lhs = buf[slot]

    def accumulate(rhs):
        for ref, cols in ((wq_ref, slice(0, qw)), (wk_ref, slice(qw, qw + kw)), (wv_ref, slice(qw + kw, qw + 2 * kw))):
            part = mm(lhs, rhs[:, cols], TN)

            @pl.when(step == 0)
            def _(ref=ref, part=part):
                ref[...] = part

            @pl.when(step > 0)
            def _(ref=ref, part=part):
                ref[...] += part

    @pl.when(step % 2 == 0)
    def _():
        accumulate(grads[0])

    @pl.when(step % 2 == 1)
    def _():
        accumulate(grads[1])


def weight_grad_in(table, normed, grads, shapes, rel, prev):
    seq, width = normed[0].shape
    block = grads[0].shape[1]
    half = width // 2
    tile = 896
    hbm = pl.BlockSpec(memory_space=pl.ANY)
    widths = [w // 4 for w in shapes]
    in_specs = [hbm] * 8 + [
        pl.BlockSpec((seq, block), lambda m, k, s: (s[S_PEER + k // 2], 0)),
        pl.BlockSpec((seq, block), lambda m, k, s: (s[S_PEER + k // 2], 0))]
    args = [table, *normed, *grads]
    alias = {}
    if prev is not None:
        in_specs += [hbm] * 3
        alias = {len(args) + idx: idx for idx in range(3)}
        args += list(prev)
    return pl.pallas_call(
        dw_in_kernel,
        grid_spec=pltpu.PrefetchScalarGridSpec(
            num_scalar_prefetch=1, grid=(half // tile, 8),
            in_specs=in_specs,
            out_specs=[pl.BlockSpec((tile, w), lambda m, k, s: (m, s[S_BLOCK + rel])) for w in widths],
            scratch_shapes=[pltpu.VMEM((2, seq, tile), BF16), pltpu.SemaphoreType.DMA((2,))],
        ),
        out_shape=[jax.ShapeDtypeStruct((half, w), F32) for w in shapes],
        input_output_aliases=alias,
        compiler_params=params(2),
        cost_estimate=cost(2 * 8 * seq * half * block, 16 * seq * half + 3 * 16 * seq * block + 4 * half * block),
        name="weight_grad_in",
    )(*args)


def dw_out_kernel(s_ref, *refs):
    n_piece = 8
    pieces, outs = refs[:n_piece], refs[n_piece:n_piece + 2]
    dw_ref, buf, sems = refs[-3:]
    n_idx, step = pl.program_id(0), pl.program_id(1)
    tile = buf.shape[2]
    slot = (n_idx * n_piece + step) % 2

    def columns(n):
        return pl.ds(pl.multiple_of(n * tile, tile), tile)

    @pl.when((n_idx == 0) & (step == 0))
    def _():
        stream(pieces, columns(0), buf, sems, step, slot)

    @pl.when(step < n_piece - 1)
    def _():
        stream(pieces, columns(n_idx), buf, sems, step + 1, 1 - slot)

    @pl.when((step == n_piece - 1) & (n_idx < pl.num_programs(0) - 1))
    def _():
        stream(pieces, columns(n_idx + 1), buf, sems, 0, 1 - slot)

    pltpu.make_async_copy(pieces[0].at[:, columns(0)], buf.at[slot], sems.at[slot]).wait()
    rhs = buf[slot]

    for which in range(2):
        @pl.when((step % 2 == which) & (step == 0))
        def _(lhs=outs[which]):
            dw_ref[...] = mm(lhs[...], rhs, TN)

        @pl.when((step % 2 == which) & (step > 0))
        def _(lhs=outs[which]):
            dw_ref[...] += mm(lhs[...], rhs, TN)


def weight_grad_out(table, d_attn, outs, rel, prev):
    seq, width = d_attn[0].shape
    depth = outs[0].shape[1]
    tile = width // 3
    hbm = pl.BlockSpec(memory_space=pl.ANY)
    in_specs = [hbm] * 8 + [
        pl.BlockSpec((seq, depth), lambda n, k, s: (s[S_PEER + k // 2], 0)),
        pl.BlockSpec((seq, depth), lambda n, k, s: (s[S_PEER + k // 2], 0))]
    args = [table, *d_attn, *outs]
    alias = {}
    if prev is not None:
        in_specs.append(hbm)
        alias = {len(args): 0}
        args.append(prev)
    return pl.pallas_call(
        dw_out_kernel,
        grid_spec=pltpu.PrefetchScalarGridSpec(
            num_scalar_prefetch=1, grid=(width // tile, 8),
            in_specs=in_specs,
            out_specs=pl.BlockSpec((depth, tile), lambda n, k, s: ((s[S_X] + rel // 2) % 2, n)),
            scratch_shapes=[pltpu.VMEM((2, seq, tile), BF16), pltpu.SemaphoreType.DMA((2,))],
        ),
        out_shape=jax.ShapeDtypeStruct((2 * depth, width), F32),
        input_output_aliases=alias,
        compiler_params=params(2),
        cost_estimate=cost(2 * 8 * seq * width * depth, 16 * seq * width + 48 * seq * depth + 4 * depth * width),
        name="weight_grad_out",
    )(*args)


def solution(mesh):
    n_cp = mesh.shape['cp']
    hops = {rel: [(dev, dev ^ rel) for dev in range(n_cp)] for rel in range(1, n_cp)}
    cores = [[0, 1], [2, 3]]

    def per_device(hidden, cotangent, pos_loc, w_q, w_k, w_v, w_o, w_pre, w_post, q_norm, k_norm):
        dim = q_norm.shape[0]
        n_batch, seq, width = hidden.shape
        kv = w_k.shape[1] // dim // n_cp
        groups = w_q.shape[1] // w_k.shape[1]
        depth = kv * groups * dim
        dev, tp = lax.axis_index('cp'), lax.axis_index('tp')
        core, x_idx = dev % 2, dev // 2
        peers = [dev ^ rel for rel in range(n_cp)]
        blocks = [2 * (p % 2) + p // 2 for p in peers]
        table = jnp.stack([jnp.asarray(v, jnp.int32) for v in [dev, tp, core, x_idx] + peers + blocks])

        def move(val, rel):
            return lax.ppermute(val, 'cp', hops[rel])

        def swap(val):
            return lax.ppermute(val, 'tp', [(0, 1), (1, 0)])

        pre2, post2 = w_pre[None, :], w_post[None, :]
        qn2, kn2 = q_norm[None, :], k_norm[None, :]

        far_half = swap(lax.dynamic_slice(w_o, (core * 2 * depth, 0), (2 * depth, width)))
        w_far = jnp.concatenate([far_half, move(far_half, 1)], axis=0)

        pos_all = lax.all_gather(pos_loc, 'cp', tiled=True).reshape(n_cp, 2, seq // 2)
        pos_log = jnp.concatenate([pos_all[:, 0].reshape(-1), pos_all[::-1, 1].reshape(-1)])
        inv_freq = 1.0 / (ROPE_SCALE * ROPE_BASE ** (jnp.arange(dim // 2, dtype=F32) * (2.0 / dim)))
        angles = pos_log.astype(F32)[:, None] * inv_freq[None, :]
        cos_t, sin_t = jnp.cos(angles), jnp.sin(angles)
        cos2 = jnp.concatenate([cos_t, cos_t], axis=1)
        sin2 = jnp.concatenate([-sin_t, sin_t], axis=1)

        normed, raws, outs, lses, lhs_own, lhs_far = [], [], [], [], [], []
        for b in range(n_batch):
            got = project(table, hidden, pre2, w_q, w_k, w_v, b, n_cp)
            normed.append(got[0])
            raws.append([got[1]] + [move(got[1 + rel], rel) for rel in range(1, n_cp)])

        out_x = []
        for b in range(n_batch):
            o_b, lse_b = attend(table, raws[b], cos2, sin2, qn2, kn2, dim, kv, groups)
            outs.append(o_b)
            lses.append(lse_b)
            o_x = move(o_b, 2)
            out_x.append(o_x)

            def rows(val, who):
                return lax.dynamic_slice(val, (who * seq, 0), (seq, val.shape[1]))

            side = move(jnp.concatenate([rows(o_b, peers[1]), rows(o_x, peers[1])], axis=1), 1)
            own = jnp.concatenate([rows(o_b, dev), side[:, :depth], rows(o_x, dev), side[:, depth:]], axis=1)
            lhs_own.append(own)
            lhs_far.append(swap(own))

        y_out, d_attn, d_post = None, [], 0.0
        for b in range(n_batch):
            y_out, da, dp = project_out(table, lhs_own[b], lhs_far[b], w_o, w_far, hidden, cotangent, post2, b, y_out)
            d_attn.append(da)
            d_post = d_post + jnp.sum(dp, axis=0)

        grads, gains = [], 0.0
        for b in range(n_batch):
            d_heads = heads_grad(table, d_attn[b], w_o, n_cp)
            d_blocks = [d_heads[0]] + [move(d_heads[rel], rel) for rel in range(1, n_cp)]
            g_b, gain_b = attend_back(table, raws[b], d_blocks, outs[b], lses[b], cos2, sin2, qn2, kn2, dim, kv, groups)
            g_x = move(g_b, 2)
            grads.append([g_b, move(g_b, 1), g_x, move(g_x, 1)])
            gains = gains + gain_b

        def everyone(vals):
            far = [move(v, 2) for v in vals]
            near = [move(v, 1) for v in vals]
            diag = [move(v, 1) for v in far]
            return [v for quad in zip(*[[a, b2, c2, d2] for a, b2, c2, d2 in zip(vals, near, far, diag)]) for v in quad]

        normed_all = everyone(normed)
        d_attn_all = everyone(d_attn)

        dx_full = jnp.zeros((n_batch, seq, width), BF16)
        d_pre = 0.0
        for b in range(n_batch):
            keep, send = input_grad(table, grads[b], w_q, w_k, w_v, seq)
            dx_b, dp = finish_dx(table, keep, swap(send), hidden, cotangent, pre2, b)
            d_pre = d_pre + jnp.sum(dp, axis=0)
            dx_full = lax.dynamic_update_slice(dx_full, dx_b[None], (b, tp * (seq // 2), 0))
            dx_full = lax.dynamic_update_slice(dx_full, swap(dx_b)[None], (b, (1 - tp) * (seq // 2), 0))

        d_wo = None
        for rel, os in ((0, outs), (2, out_x)):
            d_wo = weight_grad_out(table, d_attn_all, os, rel, d_wo)
        d_in = None
        for rel in (0, 2, 1, 3):
            d_in = weight_grad_in(table, normed_all, [g[rel] for g in grads],
                                  (w_q.shape[1], w_k.shape[1], w_v.shape[1]), rel, d_in)

        def join(val):
            return lax.all_gather(val, 'cp', axis_index_groups=cores, tiled=True)

        d_wo, d_wq, d_wk, d_wv = join(d_wo), join(d_in[0]), join(d_in[1]), join(d_in[2])
        d_post = jnp.where(tp == 0, d_post, 0.0)
        d_post, d_pre, d_qn, d_kn = lax.psum((d_post, d_pre, gains[0], gains[1]), ('tp', 'cp'))
        return y_out, dx_full, d_wq, d_wk, d_wv, d_wo, d_pre, d_post, d_qn, d_kn

    specs_in = (P('dp', 'cp', None), P('dp', 'cp', None), P(('dp', 'cp')), P(None, 'tp'), P(None, 'tp'), P(None, 'tp'),
                P('tp', None), P(None), P(None), P(None), P(None))
    specs_out = (P('dp', 'cp', None), P('dp', 'cp', None), P('dp', 'tp'), P('dp', 'tp'), P('dp', 'tp'),
                 P(('dp', 'tp'), None), P('dp'), P('dp'), P('dp'), P('dp'))
    return jax.shard_map(per_device, mesh=mesh, in_specs=specs_in, out_specs=specs_out, check_vma=False)
```
